32 devices in a mesh: role: 2 (over core), rep: 4 (over z), tp: 4 (over y, x).
Axes of the slice: x: 2, y: 2, z: 4, core: 2. Of those that a mesh axis runs over, the one named last changes fastest.
Arguments:
- pre_act: bfloat16 [2, 2, 64, 14784], P('role', None, 'rep', 'tp'), may hold values from -6 to 6
- next_pre: bfloat16 [2, 2, 64, 14784], P('role', None, 'rep', 'tp'), may hold values from -6 to 6
- stream: bfloat16 [2, 2, 64, 8192], P('role', None, 'tp', 'rep'), may hold values from -6 to 6
- cotangent: bfloat16 [64, 8192], P('tp', 'rep'), may hold values from -6 to 6
- weights: float32 [2, 14784, 8192], P('role', 'tp', 'rep'), may hold values from -6 to 6
- first_moment: float32 [14784, 8192], P('tp', 'rep'), may hold values from -0.18 to 0.18
- second_moment: float32 [14784, 8192], P('tp', 'rep'), may hold values from 0.0001 to 0.001
- tree_parent: int32 [2, 64], P('role', 'tp'), may hold values from 0 to 63, as said below
- tree_depth: int32 [2, 64], P('role', 'tp'), may hold values from 1 to 16, as said below
Outputs:
- first_out: bfloat16 [2, 64, 8192], P('role', 'tp', 'rep')
- next_out: bfloat16 [2, 64, 8192], P('role', 'tp', 'rep')
- new_weights: float32 [2, 14784, 8192], P('role', 'tp', 'rep')
The draws below stay inside these ranges and needn't reach their ends.
Inputs may be any that keep to these rules, and one draw needn't show every extreme that they name: `tree_parent`: each entry names a first-pass row of the same group that lies in the same aligned block of 16 rows as the entry's own row. `tree_depth`: one more than the depth of the named parent in its block's first-pass tree; in that tree every row but the block's first names an earlier row of the block as parent, and the first row has depth 0.
All inputs are finite; a program needn't handle non-finite values.
Results may differ from the reference program's by a relative error of at most 0.0041.
Values may be sent and summed in bfloat16 or wider, within the bound.
No kernel may reach another device: no remote copies, remote signals or barrier semaphores. Data moves between devices by JAX's collectives and lax.ppermute only.
A program may use at most 256 MiB of HBM per device.

```python
import math
import jax
import jax.numpy as jnp
from jax import lax

D = 8192
FF = 14784
ROW_DEV = 16
ROWS_ALL = 64


def tree_tables(key):
    base_key = jax.random.fold_in(key, 4113)
    per_group = ROWS_ALL // ROW_DEV
    blocks = 2 * per_group
    raw_bits = jax.random.randint(jax.random.fold_in(base_key, 1), (blocks, ROW_DEV), 0, 1 << 20)
    column = jnp.arange(ROW_DEV, dtype=jnp.int32)
    chain_block = (jnp.arange(blocks, dtype=jnp.int32) % per_group == 0)[:, None]
    random_parent = raw_bits % jnp.maximum(column, 1)[None, :]
    first_parent = jnp.where(chain_block, jnp.maximum(column - 1, 0)[None, :], random_parent)
    depths = [jnp.zeros((blocks,), jnp.int32)]
    for column_index in range(1, ROW_DEV):
        stacked = jnp.stack(depths, axis=1)
        found = jnp.take_along_axis(stacked, first_parent[:, column_index:column_index + 1], axis=1)
        depths.append(found[:, 0] + 1)
    first_depth = jnp.stack(depths, axis=1)
    random_chosen = jax.random.randint(jax.random.fold_in(base_key, 2), (blocks, ROW_DEV), 0, ROW_DEV)
    deepest = chain_block & (column[None, :] == 0)
    chosen = jnp.where(deepest, ROW_DEV - 1, random_chosen)
    next_depth = jnp.take_along_axis(first_depth, chosen, axis=1) + 1
    offsets = (jnp.arange(blocks, dtype=jnp.int32) % per_group * ROW_DEV)[:, None]
    return ((chosen + offsets).reshape(2, ROWS_ALL), next_depth.reshape(2, ROWS_ALL))


def draw_tree_parent(key, part):
    return tree_tables(key)[0]


def draw_tree_depth(key, part):
    return tree_tables(key)[1]


def block_scale(rng, dims, pieces, least, top_value):
    factor_of = 1.0
    for position, blocks in pieces:
        draws = jax.random.uniform(jax.random.fold_in(jax.random.fold_in(rng, 6), position), (blocks,), jnp.float32, least / len(pieces), top_value / len(pieces))
        factor_of = factor_of * jnp.repeat(jnp.exp(draws), dims[position] // blocks).reshape((-1,) + (1,) * (len(dims) - 1 - position))
    return factor_of


def normal_values(stream_key, dims, width, limit, split=(), kind=jnp.bfloat16):
    array = jax.random.normal(stream_key, dims, jnp.float32) * width
    if len(split) > 0:
        array = block_scale(stream_key, dims, split, -0.22, 0.18) * array
    return jnp.clip(array, min=-limit, max=limit).astype(kind)


def setup_inputs(seed: int = 0) -> dict:
    seeds = jax.random.split(jax.random.key(seed), 10)
    pre_act = normal_values(seeds[0], (2, 2, ROWS_ALL, FF), 1.0, 6.0, ((0, 2), (2, 4), (3, 4)))
    next_pre = normal_values(seeds[1], (2, 2, ROWS_ALL, FF), 1.0, 6.0, ((0, 2), (2, 4), (3, 4)))
    stream = normal_values(seeds[2], (2, 2, ROWS_ALL, D), 1.0, 6.0, ((0, 2), (2, 4), (3, 4)))
    cotangent = normal_values(seeds[3], (ROWS_ALL, D), 1.0, 6.0, ((0, 4), (1, 4)))
    weights = normal_values(seeds[4], (2, FF, D), 1.0, 6.0, ((0, 2), (1, 4), (2, 4)), jnp.float32)
    first_moment = normal_values(seeds[5], (FF, D), 0.03, 0.18, ((0, 4), (1, 4)), jnp.float32)
    second_moment = jnp.clip(jnp.exp(math.log(0.001) - 2.3025852 * jax.random.uniform(seeds[6], (FF, D), jnp.float32) ** block_scale(seeds[6], (FF, D), ((0, 4), (1, 4)), -0.2, 0.2)), 0.0001, 0.001)
    tree_parent = draw_tree_parent(jax.random.fold_in(seeds[9], 71), 0)
    tree_depth = draw_tree_depth(jax.random.fold_in(seeds[9], 71), 0)
    return {"pre_act": pre_act, "next_pre": next_pre, "stream": stream, "cotangent": cotangent, "weights": weights, "first_moment": first_moment, "second_moment": second_moment, "tree_parent": tree_parent, "tree_depth": tree_depth}


beta_one = 0.9
beta_two = 0.95
epsilon = 1e-08
learn_rate = 0.08
decay_rate = 0.1
correct_one = 1.0 - 0.9 ** 60
correct_two = 1.0 - 0.95 ** 60

def activate(both_halves):
    return (jax.nn.silu(both_halves[0].astype(jnp.float32)) * both_halves[1].astype(jnp.float32)).astype(jnp.bfloat16)

def adam_step(master, moment_one, moment_two, gradient):
    moment_one = beta_one * moment_one + (1.0 - beta_one) * gradient
    moment_two = beta_two * moment_two + (1.0 - beta_two) * gradient * gradient
    direction = moment_one / correct_one / (jnp.sqrt(moment_two / correct_two) + epsilon)
    return master - learn_rate * (direction + decay_rate * master)

def reference(pre_act, next_pre, stream, cotangent, weights, first_moment, second_moment, tree_parent, tree_depth):
    factor = FF ** (-0.5)
    hiddens = [activate(pre_act[member]) for member in range(2)]
    first_list = []
    for member in range(2):
        product = jnp.dot(hiddens[member], weights[member].astype(jnp.bfloat16), preferred_element_type=jnp.float32)
        first_list.append((stream[member, 0].astype(jnp.float32) + factor * product).astype(jnp.bfloat16))
    gradient = factor * lax.dot_general(hiddens[0], cotangent, (((0,), (0,)), ((), ())), preferred_element_type=jnp.float32)
    updated = adam_step(weights[0], first_moment, second_moment, gradient)
    fresh = updated.astype(jnp.bfloat16)
    next_list = []
    for member in range(2):
        product = jnp.dot(activate(next_pre[member]), fresh, preferred_element_type=jnp.float32)
        picked = jnp.take(first_list[member], tree_parent[member], axis=0).astype(jnp.float32)
        portion = 1.0 / (1.0 + tree_depth[member].astype(jnp.float32))
        total = stream[member, 1].astype(jnp.float32) + factor * product + picked * portion[:, None]
        next_list.append(total.astype(jnp.bfloat16))
    return (jnp.stack(first_list), jnp.stack(next_list), jnp.stack([updated, fresh.astype(jnp.float32)]))
```

```python
import functools

import jax
import jax.numpy as jnp
from jax import lax
from jax.experimental import pallas as pl
from jax.experimental.pallas import tpu as pltpu
from jax.sharding import PartitionSpec as P


FF = 14784

beta_one = 0.9
beta_two = 0.95
epsilon = 1e-08
learn_rate = 0.08
decay_rate = 0.1
correct_one = 1.0 - 0.9**60
correct_two = 1.0 - 0.95**60

factor = FF ** (-0.5)
ROOT = (beta_two / correct_two) ** 0.5
GRAD_ONE = (1.0 - beta_one) / beta_one * factor
GRAD_TWO = (1.0 - beta_two) / beta_two * factor * factor
STEP = learn_rate * beta_one / correct_one / ROOT
EPS = epsilon / ROOT
KEEP = 1.0 - learn_rate * decay_rate

TILE = 128
SLOTS = 4
OUT_SLOTS = 4
PIECES = 4
EARLY_TILES = 5
FAR_CHUNKS = 2
STAGE_LIMIT = 22 * 1024 * 1024
EARLY_LIMIT = 2 * 1024 * 1024
WIDE = 256


def activate(both_halves):
    return (
        jax.nn.silu(both_halves[0].astype(jnp.float32)) * both_halves[1].astype(jnp.float32)
    ).astype(jnp.bfloat16)


def tiles_of(low, high):
    return (high - low) // TILE, (high - low) % TILE


def whole_copy(copy, rows):
    source, target, sem = copy
    return pltpu.make_async_copy(source(0, rows), target(0, rows), sem)


def start_pieces(copy, rows):
    source, target, sem = copy
    piece = rows // PIECES if rows % (PIECES * 8) == 0 else rows
    for low in range(0, rows, piece):
        pltpu.make_async_copy(source(low, piece), target(low, piece), sem).start()


def part(ref, base):
    return lambda low, rows: ref.at[pl.ds(pl.multiple_of(base + low, 8), rows)]


def slot_part(ref, slot):
    return lambda low, rows: ref.at[slot, pl.ds(low, rows)]


def run_tiles(low, high, fetch, work, begin=0, before=None):
    full, rest = tiles_of(low, high)

    def start(index, rows):
        for copy in fetch(index, lax.rem(index, SLOTS), rows):
            start_pieces(copy, rows)

    def finish(index, rows):
        for copy in fetch(index, lax.rem(index, SLOTS), rows):
            whole_copy(copy, rows).wait()

    ahead = SLOTS - 1
    for index in range(begin, min(begin + ahead, full)):
        start(jnp.int32(index), TILE)
    if rest and full < begin + ahead:
        start(jnp.int32(full), rest)
    if before is not None:
        before()

    def body(index, carry):
        finish(index, TILE)

        @pl.when(index + ahead < full)
        def _():
            start(index + ahead, TILE)

        if rest and full >= begin + ahead:

            @pl.when(index + ahead == full)
            def _():
                start(jnp.int32(full), rest)

        work(index, lax.rem(index, SLOTS), TILE)
        return carry

    lax.fori_loop(begin, full, body, 0)
    if rest:
        index = jnp.int32(full)
        finish(index, rest)
        work(index, lax.rem(index, SLOTS), rest)


def each_strip(strips, strip):
    for c in range(strips):
        strip(c, 0)


def stage_kernel(plan, *refs):
    learn, first, take = plan["learn"], plan["first"], plan["take"]
    refs = list(refs)
    role, h, nx, cot, w, m1, m2 = refs[:7]
    refs = refs[7:]
    if plan["carry"]:
        acc_one_in, acc_two_in = refs[0], refs[1]
        refs = refs[3:]
    got = refs.pop(0) if take else None
    early = [refs.pop(0) for _ in range(3)] if plan["early"] else None
    past = refs.pop(0) if plan["past"] else None
    acc_one, acc_two, upd = refs[:3]
    refs = refs[3:]
    fresh = refs.pop(0) if learn else None
    w_buf, m1_buf, m2_buf, u_buf, b_buf, in_sem, out_sem, b_sem = refs
    width = cot.shape[1]
    wide = min(WIDE, width)
    strips = width // wide

    if plan["carry"]:
        acc_one[...] = acc_one_in[...]
        acc_two[...] = acc_two_in[...]
    else:
        acc_one[...] = jnp.zeros_like(acc_one)
        acc_two[...] = jnp.zeros_like(acc_two)

    def out_copy(base, index):
        slot = lax.rem(index, OUT_SLOTS)
        return slot_part(u_buf, slot), part(upd, base + index * TILE), out_sem.at[slot]

    def fresh_copy(index):
        slot = lax.rem(index, OUT_SLOTS)
        return slot_part(b_buf, slot), part(fresh, index * TILE), b_sem.at[slot]

    def drain(copy_of, low, high):
        full, rest = tiles_of(low, high)
        sizes = [TILE] * full + ([rest] if rest else [])
        for index in range(max(0, len(sizes) - OUT_SLOTS), len(sizes)):
            whole_copy(copy_of(jnp.int32(index)), sizes[index]).wait()

    def learner():
        low, high = learn

        def fetch(index, slot, rows):
            return [
                (part(src, low + index * TILE), slot_part(dst, slot), in_sem.at[slot, k])
                for k, (src, dst) in enumerate(((w, w_buf), (m1, m1_buf), (m2, m2_buf)))
            ]

        def work(index, slot, rows, held=None):
            outgoing = lax.rem(index, OUT_SLOTS)

            @pl.when(index >= OUT_SLOTS)
            def _():
                whole_copy(out_copy(low, index - OUT_SLOTS), TILE).wait()
                if plan["far"]:
                    whole_copy(fresh_copy(index - OUT_SLOTS), TILE).wait()

            lanes = pl.ds(pl.multiple_of(low + index * TILE, TILE), rows)
            here = pl.ds(0, rows)
            hb = h[:, lanes]
            nb = nx[:, lanes] if plan["second"] else None
            local_rows = pl.ds(pl.multiple_of(index * TILE, TILE), rows)

            def read(which, cols):
                if held is not None:
                    return early[which][local_rows, cols]
                return (w_buf, m1_buf, m2_buf)[which][slot, here, cols]

            def strip(c, carry):
                cols = pl.ds(c * wide, wide)
                wv = read(0, cols)
                acc_one[:, cols] += jnp.dot(
                    hb, wv.astype(jnp.bfloat16), preferred_element_type=jnp.float32
                )
                grad = lax.dot_general(
                    hb, cot[:, cols], (((0,), (0,)), ((), ())), preferred_element_type=jnp.float32
                )
                top = read(1, cols) + GRAD_ONE * grad
                square = read(2, cols) + GRAD_TWO * (grad * grad)
                low_part = square * lax.rsqrt(square) + EPS
                updated = KEEP * wv - STEP * (top / low_part)
                u_buf[outgoing, here, cols] = updated
                fb = updated.astype(jnp.bfloat16)
                if plan["far"]:
                    b_buf[outgoing, here, cols] = fb
                else:
                    fresh[local_rows, cols] = fb
                if plan["second"]:
                    acc_two[:, cols] += jnp.dot(nb, fb, preferred_element_type=jnp.float32)

            each_strip(strips, strip)
            start_pieces(out_copy(low, index), rows)
            if plan["far"]:
                start_pieces(fresh_copy(index), rows)

        def first_tiles():
            def body(index, carry):
                work(index, None, TILE, held=True)
                return carry

            if plan["early"]:
                lax.fori_loop(0, plan["early"], body, 0)
            if plan["past"]:
                second_of_past()

        run_tiles(low, high, fetch, work, plan["early"], first_tiles)
        drain(lambda index: out_copy(low, index), low, high)
        if plan["far"]:
            drain(fresh_copy, low, high)

    def second_of_past():
        start, stop = plan["past"]
        full, rest = tiles_of(start, stop)

        def work(index, rows):
            nb = nx[:, pl.ds(pl.multiple_of(start + index * TILE, TILE), rows)]

            def strip(c, carry):
                cols = pl.ds(c * wide, wide)
                fb = past[pl.ds(pl.multiple_of(index * TILE, TILE), rows), cols]
                acc_two[:, cols] += jnp.dot(nb, fb, preferred_element_type=jnp.float32)

            each_strip(strips, strip)

        def body(index, carry):
            work(index, TILE)
            return carry

        lax.fori_loop(0, full, body, 0)
        if rest:
            work(jnp.int32(full), rest)

    def rollout_first():
        low, high = first

        def fetch(index, slot, rows):
            return [(part(w, low + index * TILE), slot_part(w_buf, slot), in_sem.at[slot, 0])]

        def work(index, slot, rows):
            hb = h[:, pl.ds(pl.multiple_of(low + index * TILE, TILE), rows)]

            def strip(c, carry):
                cols = pl.ds(c * wide, wide)
                acc_one[:, cols] += jnp.dot(
                    hb,
                    w_buf[slot, pl.ds(0, rows), cols].astype(jnp.bfloat16),
                    preferred_element_type=jnp.float32,
                )
                return carry

            each_strip(strips, strip)

        run_tiles(low, high, fetch, work)

    def rollout_take():
        low, high = take
        full, rest = tiles_of(low, high)

        def work(index, slot, rows):
            outgoing = lax.rem(index, OUT_SLOTS)

            @pl.when(index >= OUT_SLOTS)
            def _():
                whole_copy(out_copy(low, index - OUT_SLOTS), TILE).wait()

            nb = nx[:, pl.ds(pl.multiple_of(low + index * TILE, TILE), rows)]

            def strip(c, carry):
                cols = pl.ds(c * wide, wide)
                if plan["take_far"]:
                    fb = b_buf[slot, pl.ds(0, rows), cols]
                else:
                    fb = got[pl.ds(pl.multiple_of(index * TILE, TILE), rows), cols]
                u_buf[outgoing, pl.ds(0, rows), cols] = fb.astype(jnp.float32)
                acc_two[:, cols] += jnp.dot(nb, fb, preferred_element_type=jnp.float32)

            each_strip(strips, strip)
            start_pieces(out_copy(low, index), rows)

        if plan["take_far"]:

            def fetch(index, slot, rows):
                return [(part(got, index * TILE), slot_part(b_buf, slot), in_sem.at[slot, 0])]

            run_tiles(low, high, fetch, work)
        else:

            def body(index, carry):
                work(index, None, TILE)
                return carry

            lax.fori_loop(0, full, body, 0)
            if rest:
                work(jnp.int32(full), None, rest)
        drain(lambda index: out_copy(low, index), low, high)

    if learn:
        pl.when(role[0] == 0)(learner)
    if first:
        pl.when(role[0] == 1)(rollout_first)
    if take:
        pl.when(role[0] == 1)(rollout_take)


def early_kernel(w, m1, m2, w_out, m1_out, m2_out, sems):
    rows = w_out.shape[0]
    copies = [
        (part(src, 0), part(dst, 0), sems.at[k])
        for k, (src, dst) in enumerate(((w, w_out), (m1, m1_out), (m2, m2_out)))
    ]
    for low in range(0, rows, TILE):
        for source, target, sem in copies:
            pltpu.make_async_copy(source(low, TILE), target(low, TILE), sem).start()
    for copy in copies:
        whole_copy(copy, rows).wait()


def fetch_early(tiles, w, m1, m2):
    shape = pltpu.VMEM((tiles * TILE, w.shape[1]), jnp.float32)
    size = 12 * tiles * TILE * w.shape[1]
    return pl.pallas_call(
        early_kernel,
        out_shape=[shape] * 3,
        in_specs=[pl.BlockSpec(memory_space=pl.ANY)] * 3,
        out_specs=[pl.BlockSpec(memory_space=pltpu.VMEM)] * 3,
        scratch_shapes=[pltpu.SemaphoreType.DMA((3,))],
        compiler_params=pltpu.CompilerParams(vmem_limit_bytes=EARLY_LIMIT),
        cost_estimate=pl.CostEstimate(flops=size * 16, bytes_accessed=2 * size, transcendentals=0),
    )(w, m1, m2)


def stage(plan, role, h, nx, cot, w, m1, m2, state, got, early, past):
    rows, width = h.shape[0], cot.shape[1]
    height = w.shape[0]
    vmem = pl.BlockSpec(memory_space=pltpu.VMEM)
    hbm = pl.BlockSpec(memory_space=pl.ANY)
    args = [role, h, nx, cot, w, m1, m2]
    specs = [pl.BlockSpec(memory_space=pltpu.SMEM)] + [vmem] * 3 + [hbm] * 3
    alias = {}
    if state is not None:
        args += list(state)
        specs += [vmem, vmem, hbm]
        alias = {9: 2}
    if plan["take"]:
        if plan["take_far"]:
            got = pltpu.with_memory_space_constraint(got, pltpu.HBM)
        args.append(got)
        specs.append(hbm if plan["take_far"] else vmem)
    if early is not None:
        args += early
        specs += [vmem] * 3
    if past is not None:
        args.append(past)
        specs.append(vmem)
    out = [
        jax.ShapeDtypeStruct((rows, width), jnp.float32),
        jax.ShapeDtypeStruct((rows, width), jnp.float32),
        jax.ShapeDtypeStruct((height, width), jnp.float32),
    ]
    out_specs = [vmem, vmem, hbm]
    span = 0
    if plan["learn"]:
        span = plan["learn"][1] - plan["learn"][0]
        where = pltpu.HBM if plan["far"] else pltpu.VMEM
        out.append(where((span, width), jnp.bfloat16))
        out_specs.append(hbm if plan["far"] else vmem)
    plan = dict(
        plan,
        carry=state is not None,
        early=early[0].shape[0] // TILE if early is not None else 0,
    )
    cost = pl.CostEstimate(
        flops=int(3e6 + 6 * rows * width * max(span, 64)),
        bytes_accessed=int(20 * span * width + 1e6),
        transcendentals=0,
    )
    return pl.pallas_call(
        functools.partial(stage_kernel, plan),
        out_shape=out,
        in_specs=specs,
        out_specs=out_specs,
        scratch_shapes=[
            pltpu.VMEM((SLOTS, TILE, width), jnp.float32),
            pltpu.VMEM((SLOTS, TILE, width), jnp.float32),
            pltpu.VMEM((SLOTS, TILE, width), jnp.float32),
            pltpu.VMEM((OUT_SLOTS, TILE, width), jnp.float32),
            pltpu.VMEM((OUT_SLOTS, TILE, width), jnp.bfloat16),
            pltpu.SemaphoreType.DMA((SLOTS, 3)),
            pltpu.SemaphoreType.DMA((OUT_SLOTS,)),
            pltpu.SemaphoreType.DMA((OUT_SLOTS,)),
        ],
        input_output_aliases=alias,
        compiler_params=pltpu.CompilerParams(vmem_limit_bytes=STAGE_LIMIT),
        cost_estimate=cost,
    )(*args)


def shifts_of(piece, axis):
    size = lax.axis_size(axis)
    came = []
    for by in range(1, size):
        came.append(lax.ppermute(piece, axis, [(i, (i + by) % size) for i in range(size)]))
    return came


def in_order(pieces, axis):
    size = lax.axis_size(axis)
    me = lax.axis_index(axis)
    rows, width = pieces[0].shape
    whole = jnp.zeros((rows * size, width), pieces[0].dtype)
    for by, piece in enumerate(pieces):
        whole = lax.dynamic_update_slice_in_dim(whole, piece, ((me - by) % size) * rows, 0)
    return whole


def scatter_sum(partials, axis):
    size = lax.axis_size(axis)
    if size > 4 or size & (size - 1):
        return lax.psum_scatter(partials, axis, scatter_dimension=1, tiled=True)
    rows = partials.shape[1] // size
    me = lax.axis_index(axis)
    total = lax.dynamic_slice_in_dim(partials, me * rows, rows, 1)
    sent = partials.astype(jnp.bfloat16)
    for mask in range(1, size):
        piece = lax.dynamic_slice_in_dim(sent, (me ^ mask) * rows, rows, 1)
        came = lax.ppermute(piece, axis, [(i, i ^ mask) for i in range(size)])
        total = total + came.astype(jnp.float32)
    return total


SHARES = (0.36, 0.31, 0.21, 0.12)


def cut(height):
    tiles = -(-height // TILE)
    marks = [0]
    done = 0.0
    for share in SHARES[:-1]:
        done += share
        marks.append(max(marks[-1] + 1, min(tiles, round(done * tiles))))
    marks.append(tiles)
    return [(a * TILE, min(b * TILE, height)) for a, b in zip(marks, marks[1:])]


def compute(
    pre_act,
    next_pre,
    stream,
    cotangent,
    weights,
    first_moment,
    second_moment,
    tree_parent,
    tree_depth,
):
    role = lax.axis_index("role").astype(jnp.int32).reshape(1)
    w, first_moment, second_moment = [
        pltpu.with_memory_space_constraint(array, pltpu.HBM)
        for array in (weights[0], first_moment, second_moment)
    ]
    height = w.shape[0]
    chunks = cut(height)
    count = len(chunks)

    hidden = activate(pre_act[0])
    upcoming = activate(next_pre[0])
    early = None
    if lax.axis_size("rep") > 8:
        h = lax.all_gather(hidden, "rep", axis=0, tiled=True)
        nx = lax.all_gather(upcoming, "rep", axis=0, tiled=True)
        cot_rows = lax.all_gather(cotangent, "tp", axis=0, tiled=True)
    else:
        came = shifts_of(hidden, "rep")
        cot_came = shifts_of(cotangent, "tp")
        tiles = min(EARLY_TILES, tiles_of(*chunks[0])[0])
        if tiles:
            early = fetch_early(tiles, w, first_moment, second_moment)
        h = in_order([hidden] + came, "rep")
        cot_rows = in_order([cotangent] + cot_came, "tp")
        upcoming, _ = lax.optimization_barrier((upcoming, came))
        nx = in_order([upcoming] + shifts_of(upcoming, "rep"), "rep")

    state = None
    made, flying = [], []
    for step in range(count + 2):
        far = step >= count - FAR_CHUNKS
        plan = {
            "learn": chunks[step] if step < count else None,
            "first": (0, height) if step == 0 else None,
            "take": chunks[step - 2] if step >= 2 else None,
            "second": step > 0,
            "past": chunks[0] if step == 1 else None,
            "far": far,
            "take_far": step - 2 >= count - FAR_CHUNKS,
        }
        result = stage(
            plan,
            role,
            h,
            h if step == 0 else nx,
            cot_rows,
            w,
            first_moment,
            second_moment,
            state,
            flying[step - 2] if step >= 2 else None,
            early if step == 0 else None,
            made[0] if step == 1 else None,
        )
        state = tuple(result[:3])
        if step < count:
            made.append(result[3])
            flying.append(lax.ppermute(result[3], "role", [(0, 1), (1, 0)]))
    sums = scatter_sum(jnp.stack(state[:2]), "tp")
    first_sum, next_sum = sums[0], sums[1]
    new_weights = state[2]

    first_out = (stream[0, 0].astype(jnp.float32) + factor * first_sum).astype(jnp.bfloat16)
    block_rows = first_out.shape[0]
    local_parent = tree_parent[0] - lax.axis_index("tp") * block_rows
    onehot = (local_parent[:, None] == jnp.arange(block_rows, dtype=jnp.int32)[None, :]).astype(
        jnp.bfloat16
    )
    picked = jnp.dot(onehot, first_out, preferred_element_type=jnp.float32)
    portion = 1.0 / (1.0 + tree_depth[0].astype(jnp.float32))
    total = stream[0, 1].astype(jnp.float32) + factor * next_sum + picked * portion[:, None]
    next_out = total.astype(jnp.bfloat16)
    return (first_out[None], next_out[None], new_weights[None])


def solution(mesh):
    placed = (
        P("role", None, "rep", "tp"),
        P("role", None, "rep", "tp"),
        P("role", None, "tp", "rep"),
        P("tp", "rep"),
        P("role", "tp", "rep"),
        P("tp", "rep"),
        P("tp", "rep"),
        P("role", "tp"),
        P("role", "tp"),
    )
    return jax.shard_map(
        compute,
        mesh=mesh,
        in_specs=placed,
        out_specs=(P("role", "tp", "rep"), P("role", "tp", "rep"), P("role", "tp", "rep")),
        check_vma=False,
    )
```

```python
import functools

import jax
import jax.numpy as jnp
from jax import lax
from jax.experimental import pallas as pl
from jax.experimental.pallas import tpu as pltpu
from jax.sharding import PartitionSpec as P


FF = 14784

beta_one = 0.9
beta_two = 0.95
epsilon = 1e-08
learn_rate = 0.08
decay_rate = 0.1
correct_one = 1.0 - 0.9**60
correct_two = 1.0 - 0.95**60

factor = FF ** (-0.5)
ROOT = (beta_two / correct_two) ** 0.5
GRAD_ONE = (1.0 - beta_one) / beta_one * factor
GRAD_TWO = (1.0 - beta_two) / beta_two * factor * factor
STEP = learn_rate * beta_one / correct_one / ROOT
EPS = epsilon / ROOT
KEEP = 1.0 - learn_rate * decay_rate

TILE = 128
SLOTS = 4
OUT_SLOTS = 4
PIECES = 4
EARLY_TILES = 4
FAR_CHUNKS = 0
STAGE_LIMIT = 22 * 1024 * 1024
EARLY_LIMIT = 2 * 1024 * 1024
WIDE = 256


def activate(both_halves):
    return (
        jax.nn.silu(both_halves[0].astype(jnp.float32)) * both_halves[1].astype(jnp.float32)
    ).astype(jnp.bfloat16)


def tiles_of(low, high):
    return (high - low) // TILE, (high - low) % TILE


def whole_copy(copy, rows):
    source, target, sem = copy
    return pltpu.make_async_copy(source(0, rows), target(0, rows), sem)


def start_pieces(copy, rows):
    source, target, sem = copy
    piece = rows // PIECES if rows % (PIECES * 8) == 0 else rows
    for low in range(0, rows, piece):
        pltpu.make_async_copy(source(low, piece), target(low, piece), sem).start()


def part(ref, base):
    return lambda low, rows: ref.at[pl.ds(pl.multiple_of(base + low, 8), rows)]


def slot_part(ref, slot):
    return lambda low, rows: ref.at[slot, pl.ds(low, rows)]


def run_tiles(low, high, fetch, work, begin=0, before=None):
    full, rest = tiles_of(low, high)

    def start(index, rows):
        for copy in fetch(index, lax.rem(index, SLOTS), rows):
            start_pieces(copy, rows)

    def finish(index, rows):
        for copy in fetch(index, lax.rem(index, SLOTS), rows):
            whole_copy(copy, rows).wait()

    ahead = SLOTS - 1
    for index in range(begin, min(begin + ahead, full)):
        start(jnp.int32(index), TILE)
    if rest and full < begin + ahead:
        start(jnp.int32(full), rest)
    if before is not None:
        before()

    def body(index, carry):
        finish(index, TILE)

        @pl.when(index + ahead < full)
        def _():
            start(index + ahead, TILE)

        if rest and full >= begin + ahead:

            @pl.when(index + ahead == full)
            def _():
                start(jnp.int32(full), rest)

        work(index, lax.rem(index, SLOTS), TILE)
        return carry

    lax.fori_loop(begin, full, body, 0)
    if rest:
        index = jnp.int32(full)
        finish(index, rest)
        work(index, lax.rem(index, SLOTS), rest)


def each_strip(strips, strip):
    for c in range(strips):
        strip(c, 0)


def stage_kernel(plan, *refs):
    learn, first, take = plan["learn"], plan["first"], plan["take"]
    refs = list(refs)
    role, h, nx, cot, w, m1, m2 = refs[:7]
    refs = refs[7:]
    if plan["carry"]:
        acc_one_in, acc_two_in = refs[0], refs[1]
        refs = refs[3:]
    got = refs.pop(0) if take else None
    early = [refs.pop(0) for _ in range(3)] if plan["early"] else None
    past = refs.pop(0) if plan["past"] else None
    place = refs.pop(0) if plan["final"] else None
    if plan["final"]:
        upd = refs.pop(0)
        acc_one, acc_two = refs[-2:]
        refs = refs[:-2]
        own, *pieces = [refs.pop(0) for _ in range(plan["final"])]
    else:
        acc_one, acc_two, upd = refs[:3]
        refs = refs[3:]
    fresh = refs.pop(0) if learn else None
    w_buf, m1_buf, m2_buf, u_buf, b_buf, in_sem, out_sem, b_sem = refs
    width = cot.shape[1]
    wide = min(WIDE, width)
    strips = width // wide

    if plan["carry"]:
        acc_one[...] = acc_one_in[...]
        acc_two[...] = acc_two_in[...]
    else:
        acc_one[...] = jnp.zeros_like(acc_one)
        acc_two[...] = jnp.zeros_like(acc_two)

    def out_copy(base, index):
        slot = lax.rem(index, OUT_SLOTS)
        return slot_part(u_buf, slot), part(upd, base + index * TILE), out_sem.at[slot]

    def fresh_copy(index):
        slot = lax.rem(index, OUT_SLOTS)
        return slot_part(b_buf, slot), part(fresh, index * TILE), b_sem.at[slot]

    def drain(copy_of, low, high):
        full, rest = tiles_of(low, high)
        sizes = [TILE] * full + ([rest] if rest else [])
        for index in range(max(0, len(sizes) - OUT_SLOTS), len(sizes)):
            whole_copy(copy_of(jnp.int32(index)), sizes[index]).wait()

    def learner():
        low, high = learn

        def fetch(index, slot, rows):
            return [
                (part(src, low + index * TILE), slot_part(dst, slot), in_sem.at[slot, k])
                for k, (src, dst) in enumerate(((w, w_buf), (m1, m1_buf), (m2, m2_buf)))
            ]

        def work(index, slot, rows, held=None):
            outgoing = lax.rem(index, OUT_SLOTS)

            @pl.when(index >= OUT_SLOTS)
            def _():
                whole_copy(out_copy(low, index - OUT_SLOTS), TILE).wait()
                if plan["far"]:
                    whole_copy(fresh_copy(index - OUT_SLOTS), TILE).wait()

            lanes = pl.ds(pl.multiple_of(low + index * TILE, TILE), rows)
            here = pl.ds(0, rows)
            hb = h[:, lanes]
            nb = nx[:, lanes] if plan["second"] else None
            local_rows = pl.ds(pl.multiple_of(index * TILE, TILE), rows)

            def read(which, cols):
                if held is not None:
                    return early[which][local_rows, cols]
                return (w_buf, m1_buf, m2_buf)[which][slot, here, cols]

            def strip(c, carry):
                cols = pl.ds(c * wide, wide)
                wv = read(0, cols)
                acc_one[:, cols] += jnp.dot(
                    hb, wv.astype(jnp.bfloat16), preferred_element_type=jnp.float32
                )
                grad = lax.dot_general(
                    hb, cot[:, cols], (((0,), (0,)), ((), ())), preferred_element_type=jnp.float32
                )
                top = read(1, cols) + GRAD_ONE * grad
                square = read(2, cols) + GRAD_TWO * (grad * grad)
                low_part = square * lax.rsqrt(square) + EPS
                updated = KEEP * wv - STEP * (top / low_part)
                u_buf[outgoing, here, cols] = updated
                fb = updated.astype(jnp.bfloat16)
                if plan["far"]:
                    b_buf[outgoing, here, cols] = fb
                else:
                    fresh[local_rows, cols] = fb
                if plan["second"]:
                    acc_two[:, cols] += jnp.dot(nb, fb, preferred_element_type=jnp.float32)

            each_strip(strips, strip)
            start_pieces(out_copy(low, index), rows)
            if plan["far"]:
                start_pieces(fresh_copy(index), rows)

        def first_tiles():
            def body(index, carry):
                work(index, None, TILE, held=True)
                return carry

            if plan["early"]:
                lax.fori_loop(0, plan["early"], body, 0)
            if plan["past"]:
                second_of_past()

        run_tiles(low, high, fetch, work, plan["early"], first_tiles)
        drain(lambda index: out_copy(low, index), low, high)
        if plan["far"]:
            drain(fresh_copy, low, high)

    def second_of_past():
        start, stop = plan["past"]
        full, rest = tiles_of(start, stop)

        def work(index, rows):
            nb = nx[:, pl.ds(pl.multiple_of(start + index * TILE, TILE), rows)]

            def strip(c, carry):
                cols = pl.ds(c * wide, wide)
                fb = past[pl.ds(pl.multiple_of(index * TILE, TILE), rows), cols]
                acc_two[:, cols] += jnp.dot(nb, fb, preferred_element_type=jnp.float32)

            each_strip(strips, strip)

        def body(index, carry):
            work(index, TILE)
            return carry

        lax.fori_loop(0, full, body, 0)
        if rest:
            work(jnp.int32(full), rest)

    def rollout_first():
        low, high = first

        def fetch(index, slot, rows):
            return [(part(w, low + index * TILE), slot_part(w_buf, slot), in_sem.at[slot, 0])]

        def work(index, slot, rows):
            hb = h[:, pl.ds(pl.multiple_of(low + index * TILE, TILE), rows)]

            def strip(c, carry):
                cols = pl.ds(c * wide, wide)
                acc_one[:, cols] += jnp.dot(
                    hb,
                    w_buf[slot, pl.ds(0, rows), cols].astype(jnp.bfloat16),
                    preferred_element_type=jnp.float32,
                )
                return carry

            each_strip(strips, strip)

        run_tiles(low, high, fetch, work)

    def rollout_take():
        low, high = take
        full, rest = tiles_of(low, high)

        def work(index, slot, rows):
            outgoing = lax.rem(index, OUT_SLOTS)

            @pl.when(index >= OUT_SLOTS)
            def _():
                whole_copy(out_copy(low, index - OUT_SLOTS), TILE).wait()

            nb = nx[:, pl.ds(pl.multiple_of(low + index * TILE, TILE), rows)]

            def strip(c, carry):
                cols = pl.ds(c * wide, wide)
                if plan["take_far"]:
                    fb = b_buf[slot, pl.ds(0, rows), cols]
                else:
                    fb = got[pl.ds(pl.multiple_of(index * TILE, TILE), rows), cols]
                u_buf[outgoing, pl.ds(0, rows), cols] = fb.astype(jnp.float32)
                acc_two[:, cols] += jnp.dot(nb, fb, preferred_element_type=jnp.float32)

            each_strip(strips, strip)
            start_pieces(out_copy(low, index), rows)

        if plan["take_far"]:

            def fetch(index, slot, rows):
                return [(part(got, index * TILE), slot_part(b_buf, slot), in_sem.at[slot, 0])]

            run_tiles(low, high, fetch, work)
        else:

            def body(index, carry):
                work(index, None, TILE)
                return carry

            lax.fori_loop(0, full, body, 0)
            if rest:
                work(jnp.int32(full), None, rest)
        drain(lambda index: out_copy(low, index), low, high)

    if learn:
        pl.when(role[0] == 0)(learner)
    if first:
        pl.when(role[0] == 1)(rollout_first)
    if take:
        pl.when(role[0] == 1)(rollout_take)
    if plan["final"]:
        size = own.shape[1]
        for which, acc in enumerate((acc_one, acc_two)):
            for mask in range(plan["final"]):
                rows = pl.ds(pl.multiple_of((place[0] ^ mask) * size, 8), size)
                if mask:
                    pieces[mask - 1][which] = acc[rows, :].astype(jnp.bfloat16)
                else:
                    own[which] = acc[rows, :]


def early_kernel(w, m1, m2, w_out, m1_out, m2_out, sems):
    rows = w_out.shape[0]
    copies = [
        (part(src, 0), part(dst, 0), sems.at[k])
        for k, (src, dst) in enumerate(((w, w_out), (m1, m1_out), (m2, m2_out)))
    ]
    for low in range(0, rows, TILE):
        for source, target, sem in copies:
            pltpu.make_async_copy(source(low, TILE), target(low, TILE), sem).start()
    for copy in copies:
        whole_copy(copy, rows).wait()


def fetch_early(tiles, w, m1, m2):
    shape = pltpu.VMEM((tiles * TILE, w.shape[1]), jnp.float32)
    size = 12 * tiles * TILE * w.shape[1]
    return pl.pallas_call(
        early_kernel,
        out_shape=[shape] * 3,
        in_specs=[pl.BlockSpec(memory_space=pl.ANY)] * 3,
        out_specs=[pl.BlockSpec(memory_space=pltpu.VMEM)] * 3,
        scratch_shapes=[pltpu.SemaphoreType.DMA((3,))],
        compiler_params=pltpu.CompilerParams(vmem_limit_bytes=EARLY_LIMIT),
        cost_estimate=pl.CostEstimate(flops=size * 16, bytes_accessed=2 * size, transcendentals=0),
    )(w, m1, m2)


def stage(plan, role, h, nx, cot, w, m1, m2, state, got, early, past, place):
    rows, width = h.shape[0], cot.shape[1]
    height = w.shape[0]
    vmem = pl.BlockSpec(memory_space=pltpu.VMEM)
    hbm = pl.BlockSpec(memory_space=pl.ANY)
    args = [role, h, nx, cot, w, m1, m2]
    specs = [pl.BlockSpec(memory_space=pltpu.SMEM)] + [vmem] * 3 + [hbm] * 3
    alias = {}
    if state is not None:
        args += list(state)
        specs += [vmem, vmem, hbm]
        alias = {9: 2}
    if plan["take"]:
        if plan["take_far"]:
            got = pltpu.with_memory_space_constraint(got, pltpu.HBM)
        args.append(got)
        specs.append(hbm if plan["take_far"] else vmem)
    if early is not None:
        args += early
        specs += [vmem] * 3
    if past is not None:
        args.append(past)
        specs.append(vmem)
    if plan["final"]:
        args.append(place)
        specs.append(pl.BlockSpec(memory_space=pltpu.SMEM))
    out = [
        jax.ShapeDtypeStruct((rows, width), jnp.float32),
        jax.ShapeDtypeStruct((rows, width), jnp.float32),
        jax.ShapeDtypeStruct((height, width), jnp.float32),
    ]
    out_specs = [vmem, vmem, hbm]
    span = 0
    if plan["learn"]:
        span = plan["learn"][1] - plan["learn"][0]
        where = pltpu.HBM if plan["far"] else pltpu.VMEM
        out.append(where((span, width), jnp.bfloat16))
        out_specs.append(hbm if plan["far"] else vmem)
    sums = []
    if plan["final"]:
        out, out_specs, alias = out[2:], out_specs[2:], {9: 0}
        sums = [pltpu.VMEM((rows, width), jnp.float32)] * 2
        piece = (2, rows // plan["final"], width)
        out.append(jax.ShapeDtypeStruct(piece, jnp.float32))
        out += [jax.ShapeDtypeStruct(piece, jnp.bfloat16)] * (plan["final"] - 1)
        out_specs += [vmem] * plan["final"]
    plan = dict(
        plan,
        carry=state is not None,
        early=early[0].shape[0] // TILE if early is not None else 0,
    )
    cost = pl.CostEstimate(
        flops=int(3e6 + 6 * rows * width * max(span, 64)),
        bytes_accessed=int(20 * span * width + 1e6),
        transcendentals=0,
    )
    return pl.pallas_call(
        functools.partial(stage_kernel, plan),
        out_shape=out,
        in_specs=specs,
        out_specs=out_specs,
        scratch_shapes=[
            pltpu.VMEM((SLOTS, TILE, width), jnp.float32),
            pltpu.VMEM((SLOTS, TILE, width), jnp.float32),
            pltpu.VMEM((SLOTS, TILE, width), jnp.float32),
            pltpu.VMEM((OUT_SLOTS, TILE, width), jnp.float32),
            pltpu.VMEM((OUT_SLOTS, TILE, width), jnp.bfloat16),
            pltpu.SemaphoreType.DMA((SLOTS, 3)),
            pltpu.SemaphoreType.DMA((OUT_SLOTS,)),
            pltpu.SemaphoreType.DMA((OUT_SLOTS,)),
        ]
        + sums,
        input_output_aliases=alias,
        compiler_params=pltpu.CompilerParams(vmem_limit_bytes=STAGE_LIMIT),
        cost_estimate=cost,
    )(*args)


def shifts_of(piece, axis):
    size = lax.axis_size(axis)
    came = []
    for by in range(1, size):
        came.append(lax.ppermute(piece, axis, [(i, (i + by) % size) for i in range(size)]))
    return came


def in_order(pieces, axis):
    size = lax.axis_size(axis)
    me = lax.axis_index(axis)
    rows, width = pieces[0].shape
    whole = jnp.zeros((rows * size, width), pieces[0].dtype)
    for by, piece in enumerate(pieces):
        whole = lax.dynamic_update_slice_in_dim(whole, piece, ((me - by) % size) * rows, 0)
    return whole


def exchange(own, pieces, axis):
    for mask, piece in enumerate(pieces, 1):
        size = lax.axis_size(axis)
        own = own + lax.ppermute(piece, axis, [(i, i ^ mask) for i in range(size)])
    return own


SHARES = (0.36, 0.31, 0.21, 0.12)


def cut(height):
    tiles = -(-height // TILE)
    marks = [0]
    done = 0.0
    for share in SHARES[:-1]:
        done += share
        marks.append(max(marks[-1] + 1, min(tiles, round(done * tiles))))
    marks.append(tiles)
    return [(a * TILE, min(b * TILE, height)) for a, b in zip(marks, marks[1:])]


def compute(
    pre_act,
    next_pre,
    stream,
    cotangent,
    weights,
    first_moment,
    second_moment,
    tree_parent,
    tree_depth,
):
    role = lax.axis_index("role").astype(jnp.int32).reshape(1)
    w, first_moment, second_moment = [
        pltpu.with_memory_space_constraint(array, pltpu.HBM)
        for array in (weights[0], first_moment, second_moment)
    ]
    height = w.shape[0]
    chunks = cut(height)
    count = len(chunks)

    hidden = activate(pre_act[0])
    upcoming = activate(next_pre[0])
    early = None
    if lax.axis_size("rep") > 8:
        h = lax.all_gather(hidden, "rep", axis=0, tiled=True)
        nx = lax.all_gather(upcoming, "rep", axis=0, tiled=True)
        cot_rows = lax.all_gather(cotangent, "tp", axis=0, tiled=True)
    else:
        came = shifts_of(hidden, "rep")
        cot_came = shifts_of(cotangent, "tp")
        tiles = min(EARLY_TILES, tiles_of(*chunks[0])[0])
        if tiles:
            early = fetch_early(tiles, w, first_moment, second_moment)
        h = in_order([hidden] + came, "rep")
        cot_rows = in_order([cotangent] + cot_came, "tp")
        upcoming, _ = lax.optimization_barrier((upcoming, came))
        nx = in_order([upcoming] + shifts_of(upcoming, "rep"), "rep")

    state = None
    made, flying = [], []
    others = lax.axis_size("tp") - 1 if lax.axis_size("tp") in (2, 4) else 0
    place = lax.axis_index("tp").astype(jnp.int32).reshape(1)
    for step in range(count + 2):
        far = step >= count - FAR_CHUNKS
        plan = {
            "learn": chunks[step] if step < count else None,
            "first": (0, height) if step == 0 else None,
            "take": chunks[step - 2] if step >= 2 else None,
            "second": step > 0,
            "past": chunks[0] if step == 1 else None,
            "far": far,
            "final": others + 1 if others and step == count + 1 else 0,
            "take_far": step - 2 >= count - FAR_CHUNKS,
        }
        result = stage(
            plan,
            role,
            h,
            h if step == 0 else nx,
            cot_rows,
            w,
            first_moment,
            second_moment,
            state,
            flying[step - 2] if step >= 2 else None,
            early if step == 0 else None,
            made[0] if step == 1 else None,
            place,
        )
        state = tuple(result[:3])
        if step < count:
            made.append(result[3])
            flying.append(lax.ppermute(result[3], "role", [(0, 1), (1, 0)]))
    if others:
        new_weights = result[0]
        sums = exchange(result[1], result[2:], "tp")
    else:
        new_weights = state[2]
        sums = lax.psum_scatter(jnp.stack(state[:2]), "tp", scatter_dimension=1, tiled=True)
    first_sum, next_sum = sums[0], sums[1]

    first_out = (stream[0, 0].astype(jnp.float32) + factor * first_sum).astype(jnp.bfloat16)
    block_rows = first_out.shape[0]
    local_parent = lax.rem(tree_parent[0], jnp.int32(block_rows))
    onehot = (local_parent[:, None] == jnp.arange(block_rows, dtype=jnp.int32)[None, :]).astype(
        jnp.bfloat16
    )
    picked = jnp.dot(onehot, first_out, preferred_element_type=jnp.float32)
    portion = 1.0 / (1.0 + tree_depth[0].astype(jnp.float32))
    total = stream[0, 1].astype(jnp.float32) + factor * next_sum + picked * portion[:, None]
    next_out = total.astype(jnp.bfloat16)
    return (first_out[None], next_out[None], new_weights[None])


def solution(mesh):
    placed = (
        P("role", None, "rep", "tp"),
        P("role", None, "rep", "tp"),
        P("role", None, "tp", "rep"),
        P("tp", "rep"),
        P("role", "tp", "rep"),
        P("tp", "rep"),
        P("tp", "rep"),
        P("role", "tp"),
        P("role", "tp"),
    )
    return jax.shard_map(
        compute,
        mesh=mesh,
        in_specs=placed,
        out_specs=(P("role", "tp", "rep"), P("role", "tp", "rep"), P("role", "tp", "rep")),
        check_vma=False,
    )
```
